32 devices in a mesh: node: 8 (over z, y), local: 4 (over x, core).
Axes of the slice: x: 2, y: 2, z: 4, core: 2. Of those that a mesh axis runs over, the one named last changes fastest.
Arguments:
- tokens: bfloat16 [4096, 7168], P(('node', 'local')), may hold values from -6 to 6
- w_gate: bfloat16 [8, 7168, 1024], P('node', None, 'local'), may hold values from -0.0625 to 0.0625
- w_up: bfloat16 [8, 7168, 1024], P('node', None, 'local'), may hold values from -0.0625 to 0.0625
- w_down: bfloat16 [8, 1024, 7168], P('node', 'local'), may hold values from -0.1875 to 0.1875
- chosen: int32 [8, 48], replicated, may hold values from 0 to 4095, as said below
- counts: int32 [8], replicated, may hold values from 3 to 48, as said below
- gates: float32 [8, 48], replicated, may hold values from 0.2 to 1
Outputs:
- mixed: bfloat16 [4096, 7168], P(('node', 'local'))
The draws below stay inside these ranges and needn't reach their ends.
Inputs may be any that keep to these rules, and one draw needn't show every extreme that they name: `chosen`: each expert's list holds distinct tokens; in each list at most 3 entries lie in one device's block of 128 consecutive tokens, and for every expert some block holds exactly 3 live entries. `counts`: some expert has exactly 48 live entries.
All inputs are finite; a program needn't handle non-finite values.
Results may differ from the reference program's by a relative error of at most 0.014.
Values may be sent and summed in bfloat16 or wider, within the bound.
A program may use at most 128 MiB of HBM per device.

```python
import jax
import jax.numpy as jnp
from jax import lax

D = 7168
FF = 1024
SLOT = 3
TOK_DEV = 128
EXPERTS = 8
TOKENS = 4096
CAP = 48
FF_DEV = 256
N_LOCAL = 4


def lists_for(key):
    base = jax.random.fold_in(key, 11)
    many = TOKENS // TOK_DEV

    def one_list(index):
        sub = jax.random.fold_in(base, index)
        first, second, third, fourth = jax.random.split(sub, 4)
        heavy = jax.random.randint(first, (), 0, many)
        places = jnp.arange(many * SLOT, dtype=jnp.int32)
        owner = places // SLOT
        ranks = jax.random.permutation(second, many * SLOT).astype(jnp.int32)
        score = ranks - jnp.where(owner == heavy, many * SLOT, 0)
        order = jnp.argsort(score, stable=True)[:CAP]
        within = jax.random.permutation(third, TOK_DEV)[:SLOT].astype(jnp.int32)
        offsets = jax.random.randint(fourth, (many,), 0, TOK_DEV)
        position = (within[places % SLOT] + offsets[owner]) % TOK_DEV
        token = owner * TOK_DEV + position
        return token[order].astype(jnp.int32)
    return jax.vmap(one_list)(jnp.arange(EXPERTS, dtype=jnp.int32))


def draw_chosen(key, part):
    return lists_for(key)


def draw_counts(key, part):
    sub = jax.random.fold_in(key, 23)
    first, second = jax.random.split(sub)
    values = jax.random.randint(first, (EXPERTS,), 3 * CAP // 4, CAP + 1)
    full = jax.random.randint(second, (), 0, EXPERTS)
    return jnp.where(jnp.arange(EXPERTS) == full, CAP, values).astype(jnp.int32)


def shard_levels(own_key, shape, cuts, least, largest):
    gain, own = 1.0, jax.random.fold_in(own_key, 6)
    for axis_at, blocks in cuts:
        steps = jnp.exp(jax.random.uniform(jax.random.fold_in(own, axis_at), (blocks,), jnp.float32, least / len(cuts), largest / len(cuts)))
        gain = gain * jnp.repeat(steps, shape[axis_at] // blocks).reshape([-1 if axis == axis_at else 1 for axis in range(len(shape))])
    return gain


def gaussian(own_key, extent, width, limit, cuts=(), held_as=jnp.bfloat16):
    entries = jax.random.normal(own_key, extent, jnp.float32) * width
    if len(cuts) > 0:
        entries = shard_levels(own_key, extent, cuts, -0.22, 0.18) * entries
    return jnp.clip(entries, min=-limit, max=limit).astype(held_as)


def setup_inputs(seed: int = 0) -> dict:
    keys = jax.random.split(jax.random.key(seed), 8)
    return {
        "tokens": gaussian(keys[0], (TOKENS, D), 1.0, 6.0, ((0, 32),)),
        "w_gate": gaussian(keys[1], (EXPERTS, D, FF), D ** -0.5, 0.0625, ((0, 8), (2, 4))),
        "w_up": gaussian(keys[2], (EXPERTS, D, FF), D ** -0.5, 0.0625, ((0, 8), (2, 4))),
        "w_down": gaussian(keys[3], (EXPERTS, FF, D), FF ** -0.5, 0.1875, ((0, 8), (1, 4))),
        "chosen": draw_chosen(jax.random.fold_in(keys[7], 71), 0),
        "counts": draw_counts(jax.random.fold_in(keys[7], 71), 0),
        "gates": jnp.clip(jax.random.uniform(keys[6], (EXPERTS, CAP), jnp.float32, 0.2, 1.0), 0.2, 1.0),
    }


def reference(tokens, w_gate, w_up, w_down, chosen, counts, gates):
    def one_expert(total, item):
        gate_mat, up_mat, down_mat, picked, count, weight = item
        rows = tokens[picked]
        live = jnp.arange(CAP, dtype=jnp.int32) < count
        scale = jnp.where(live, weight, jnp.float32(0.0))
        answer = jnp.zeros((CAP, D), jnp.float32)
        for group in range(N_LOCAL):
            low = group * FF_DEV
            gate_val = jnp.dot(rows, gate_mat[:, low:low + FF_DEV], preferred_element_type=jnp.float32)
            up_val = jnp.dot(rows, up_mat[:, low:low + FF_DEV], preferred_element_type=jnp.float32)
            hidden = (jax.nn.silu(gate_val) * up_val).astype(jnp.bfloat16)
            down_val = jnp.dot(hidden, down_mat[low:low + FF_DEV, :], preferred_element_type=jnp.float32)
            part = (scale[:, None] * down_val).astype(jnp.bfloat16)
            answer = answer + part.astype(jnp.float32)
        answer = answer.astype(jnp.bfloat16).astype(jnp.float32)
        answer = jnp.where(live[:, None], answer, jnp.float32(0.0))
        return total.at[picked].add(answer), None

    start = jnp.zeros((TOKENS, D), jnp.float32)
    total, _ = lax.scan(one_expert, start, (w_gate, w_up, w_down, chosen, counts, gates))
    return total.astype(jnp.bfloat16)
```

```python
import functools

import jax
import jax.numpy as jnp
from jax import lax
from jax.experimental import pallas as pl
from jax.experimental.pallas import tpu as pltpu
from jax.sharding import PartitionSpec as P

SLOT = 3
SUB, LANE = 8, 128
COLS = SUB * LANE
MESH = pl.DeviceIdType.MESH
BATCHES = 3
DISPATCH_GROUPS = 2
COMBINE_GROUPS = 2


def split(count, groups):
    groups = min(groups, count)
    sizes = [count // groups + (1 if g < count % groups else 0) for g in range(groups)]
    starts = [sum(sizes[:g]) for g in range(groups)]
    return list(zip(starts, sizes))


def row_order(n_node):
    far = [(k, s) for k in range(n_node - 1, n_node // 2 - 1, -1) for s in range(SLOT)]
    near = [(k, s) for k in range(n_node // 2 - 1, -1, -1) for s in range(SLOT)]
    half, rows = SUB // 2, []
    while far or near:
        rows += far[:half] + near[:half]
        far, near = far[half:], near[half:]
    return rows


def runs_of(order, first, count):
    runs = []
    for p in range(first, first + count):
        k = order[p][0]
        if runs and runs[-1][0] == k and runs[-1][1] + runs[-1][2] == p:
            runs[-1][2] += 1
        else:
            runs.append([k, p, 1])
    return [tuple(run) for run in runs]


def plan(nb, dg, cg):
    wire = 7.4 / (nb * dg)
    steps = []
    done = {}
    for b in range(nb):
        for g in range(dg):
            i = b * dg + g
            near = 2.2 + wire * (i + 1)
            across = near + 1.8 + wire
            steps.append((near, "pass_on", b, g))
            steps.append((across, "pass_across", b, g))
            steps.append((across + 1.1, "hidden", b, g))
            done[b] = across + 1.1
        start = done[b] + 0.4
        steps.append((start, "down", b, 0))
        for g in range(cg):
            steps.append((start + 1.0 + 0.3 * g, "pair_sum", b, g))
            steps.append((start + 3.4 + 1.2 * g, "answer", b, g))
    return [step[1:] for step in sorted(steps, key=lambda step: step[0])]


def kernel(dims, counts_hbm, chosen_hbm, gates_hbm, tokens_hbm, wg_hbm, wu_hbm, wd_hbm, out_ref,
           counts_ref, chosen_ref, gates_ref, tokens_ref, wg, wu, wd, tx, rx, py, r1b, s2, r2b, a3, ax, stage,
           wsem, ssem, d1, d2, d3, c1, c2, c3):
    n_node, n_local, chunks, tok_dev, ff = dims
    nx = n_local // 2
    experts, cap = chosen_ref.shape
    per = n_node * SLOT
    octs = per // SUB
    f32, bf16 = jnp.float32, jnp.bfloat16
    me_n, me_l = lax.axis_index("node"), lax.axis_index("local")
    me_x, me_c = me_l // 2, me_l % 2
    mine, half, other = me_c * nx + me_x, me_c * nx, (1 - me_c) * nx
    partner = me_x * 2 + (1 - me_c)
    order = row_order(n_node)
    batches = split(octs, BATCHES)
    dgroups, cgroups = split(chunks, DISPATCH_GROUPS), split(chunks, COMBINE_GROUPS)

    paired = n_node & (n_node - 1) == 0

    def node_at(k):
        if paired:
            return jnp.bitwise_xor(me_n, abs(k))
        return lax.rem(me_n + k + n_node, n_node)

    def x_at(k):
        return lax.rem(me_x + k + nx, nx)

    def remote(src, dst, ssem, rsem, node, local):
        return pltpu.make_async_remote_copy(
            src_ref=src, dst_ref=dst, send_sem=ssem, recv_sem=rsem,
            device_id=(node, local), device_id_type=MESH)

    def send(*args):
        remote(*args).start()

    def arrived(ref, sem):
        remote(ref, ref, sem, sem, me_n, partner).wait_recv()

    barrier = pltpu.get_barrier_semaphore()
    for k in range(1, n_node):
        pl.semaphore_signal(barrier, inc=1, device_id=(node_at(k), me_l), device_id_type=MESH)
    pl.semaphore_signal(barrier, inc=1, device_id=(me_n, partner), device_id_type=MESH)
    for k in range(1, nx):
        pl.semaphore_signal(barrier, inc=1, device_id=(me_n, x_at(k) * 2 + me_c), device_id_type=MESH)

    loads = [pltpu.make_async_copy(src, dst, wsem.at[i]) for i, (src, dst) in enumerate((
        (wg_hbm.at[0], wg), (wu_hbm.at[0], wu), (wd_hbm.at[0], wd), (tokens_hbm, tokens_ref),
        (counts_hbm, counts_ref), (chosen_hbm, chosen_ref), (gates_hbm, gates_ref)))]
    for copy in loads[4:] + [loads[3]] + loads[:3]:
        copy.start()
    for copy in loads[4:]:
        copy.wait()

    base = (me_n * n_local + me_l) * tok_dev
    row = lax.broadcasted_iota(jnp.int32, (experts, cap), 0)
    count = jnp.zeros((experts, cap), jnp.int32)
    for e in range(experts):
        count = jnp.where(row == e, counts_ref[e], count)
    pos = chosen_ref[...] - base
    live = (lax.broadcasted_iota(jnp.int32, (experts, cap), 1) < count) & (pos >= 0) & (pos < tok_dev)
    before = (lax.broadcasted_iota(jnp.int32, (cap, cap), 0)
              < lax.broadcasted_iota(jnp.int32, (cap, cap), 1))
    rank = jnp.dot(jnp.where(live, 1.0, 0.0).astype(bf16), jnp.where(before, 1.0, 0.0).astype(bf16),
                   preferred_element_type=f32)
    pos1 = (pos + 1).astype(f32)
    lane1 = (lax.broadcasted_iota(jnp.int32, (experts, tok_dev), 1) + 1).astype(f32)
    hits = []
    for s in range(SLOT):
        where = jnp.sum(jnp.where(live & (rank == float(s)), pos1, 0.0), axis=1, keepdims=True)
        hits.append(lane1 == where)
    pick = jnp.concatenate([jnp.where(hit, 1.0, 0.0) for hit in hits], axis=0)
    col = lax.broadcasted_iota(jnp.int32, (per, per), 1)
    source = lax.broadcasted_iota(jnp.int32, (per, per), 0)
    wanted = jnp.zeros((per, per), jnp.int32)
    for p, (k, s) in enumerate(order):
        wanted = jnp.where(source == p, node_at(k) + s * experts, wanted)
    permute = jnp.where(col == wanted, 1.0, 0.0).astype(bf16)

    def ordered(x):
        return jnp.dot(permute, x, preferred_element_type=f32)

    select = ordered(pick.astype(bf16)).astype(bf16)

    def to_tiles(value, m, side):
        for q in range(SUB):
            stage[side, pl.ds(q, m, stride=SUB), :] = value[:, q * LANE:(q + 1) * LANE]
        return stage[side, pl.ds(0, m * SUB), :].astype(bf16).reshape(m, SUB, LANE)

    def from_tiles(value, m, side, times=1):
        stage[side, pl.ds(0, m * SUB), :] = value.reshape(m * SUB, LANE).astype(f32)
        parts = [stage[side, pl.ds(q, m, stride=SUB), :] for q in range(SUB)]
        return jnp.concatenate([jnp.concatenate([p] * times, axis=0).astype(bf16) for p in parts], axis=1)

    def send_rows(src, dst, b, js, sems, sent, back):
        o0, on = batches[b]
        for k, p, n in runs_of(order, o0 * SUB, on * SUB):
            if k:
                send(src.at[js, pl.ds(p, n)], dst.at[js, pl.ds(p, n)] if back else dst.at[js, mine, pl.ds(p, n)],
                     sent, sems, node_at(-k if back else k), me_l)

    def remote_rows(b):
        o0, on = batches[b]
        return sum(n for k, _, n in runs_of(order, o0 * SUB, on * SUB) if k)

    def own_rows(b):
        o0, on = batches[b]
        return [(p, n) for k, p, n in runs_of(order, o0 * SUB, on * SUB) if not k]

    loads[3].wait()
    for g, (j0, jn) in enumerate(dgroups):
        for j in range(j0, j0 + jn):
            picked = jnp.dot(select, tokens_ref[:, j * COLS:(j + 1) * COLS], preferred_element_type=f32)
            tiles = to_tiles(picked, per, j % 2)
            tx[j] = tiles
            for b in range(len(batches)):
                for p, n in own_rows(b):
                    rx[j, mine, p:p + n] = tiles[p:p + n]
        if g == 0:
            pl.semaphore_wait(barrier, n_node - 1 + 1 + nx - 1)
        send_rows(tx, rx, 0, pl.ds(j0, jn), d1.at[0, g], ssem.at[0], False)
    for b in range(1, len(batches)):
        for g, (j0, jn) in enumerate(dgroups):
            send_rows(tx, rx, b, pl.ds(j0, jn), d1.at[b, g], ssem.at[0], False)

    weight = jnp.concatenate([
        jnp.where(hits[s], jnp.sum(jnp.where(live & (rank == float(s)), gates_ref[...], 0.0), axis=1, keepdims=True), 0.0)
        for s in range(SLOT)], axis=0)
    high = weight.astype(bf16)
    low = (weight - high.astype(f32)).astype(bf16)
    place = jnp.transpose(jnp.concatenate([ordered(high), ordered(low)], axis=0)).astype(bf16)

    hidden_of = {}

    def pass_on(b, g):
        o0, on = batches[b]
        js, rows = pl.ds(*dgroups[g]), pl.ds(o0 * SUB, on * SUB)
        arrived(rx.at[js, mine, pl.ds(o0 * SUB, remote_rows(b))], d1.at[b, g])
        block = rx.at[js, mine, rows]
        for d in range(1, nx):
            send(block, block, ssem.at[1], d2.at[b, g], me_n, x_at(d) * 2 + me_c)
        send(block, block, ssem.at[2], d3.at[b, g], me_n, partner)

    def pass_across(b, g):
        o0, on = batches[b]
        js, rows = pl.ds(*dgroups[g]), pl.ds(o0 * SUB, on * SUB)
        arrived(rx.at[js, pl.ds(half, nx - 1), rows], d2.at[b, g])
        for d in range(1, nx):
            block = rx.at[js, half + x_at(-d), rows]
            send(block, block, ssem.at[2], d3.at[b, g], me_n, partner)

    def hidden(b, g):
        o0, on = batches[b]
        j0, jn = dgroups[g]
        m = n_local * on * SUB
        arrived(rx.at[pl.ds(j0, jn), pl.ds(other, nx), pl.ds(o0 * SUB, on * SUB)], d3.at[b, g])
        if b == 0 and g == 0:
            loads[0].wait()
            loads[1].wait()
        x = jnp.concatenate([
            from_tiles(rx[j, :, o0 * SUB:(o0 + on) * SUB].reshape(m, SUB, LANE), m, j % 2)
            for j in range(j0, j0 + jn)], axis=1)
        ks = pl.ds(j0 * COLS, jn * COLS)
        now = (jnp.dot(x, wg[ks, :], preferred_element_type=f32), jnp.dot(x, wu[ks, :], preferred_element_type=f32))
        old = hidden_of.get(b)
        hidden_of[b] = now if old is None else (old[0] + now[0], old[1] + now[1])

    def down(b, _):
        o0, on = batches[b]
        gate, up = hidden_of.pop(b)
        h = (gate / (1.0 + jnp.exp(-gate)) * up).astype(bf16)
        if b == 0:
            loads[2].wait()
        for g, (j0, jn) in enumerate(cgroups):
            js = pl.ds(j0, jn)
            for j in range(j0, j0 + jn):
                y = jnp.dot(h, wd[:, j * COLS:(j + 1) * COLS], preferred_element_type=f32)
                py[j, :, o0:o0 + on] = y.reshape(n_local, on, SUB, COLS).astype(bf16)
            send(py.at[js, pl.ds(other, nx), pl.ds(o0, on)], r1b.at[js, :, pl.ds(o0, on)],
                 ssem.at[3], c1.at[b, g], me_n, partner)

    def pair_sum(b, g):
        o0, on = batches[b]
        j0, jn = cgroups[g]
        js, os = pl.ds(j0, jn), pl.ds(o0, on)
        arrived(r1b.at[js, :, os], c1.at[b, g])
        for d in range(1, nx):
            xd = x_at(d)
            for j in range(j0, j0 + jn):
                s2[j, d - 1, o0:o0 + on] = (py[j, half + xd, o0:o0 + on].astype(f32)
                                            + r1b[j, xd, o0:o0 + on].astype(f32)).astype(bf16)
            send(s2.at[js, d - 1, os], r2b.at[js, d - 1, os], ssem.at[4], c2.at[b, g], me_n, xd * 2 + me_c)

    def answer(b, g):
        o0, on = batches[b]
        j0, jn = cgroups[g]
        js, os = pl.ds(j0, jn), pl.ds(o0, on)
        arrived(r2b.at[js, :, os], c2.at[b, g])
        for j in range(j0, j0 + jn):
            total = py[j, mine, o0:o0 + on].astype(f32) + r1b[j, me_x, o0:o0 + on].astype(f32)
            for d in range(1, nx):
                total = total + r2b[j, d - 1, o0:o0 + on].astype(f32)
            tiles = to_tiles(total.reshape(on * SUB, COLS), on * SUB, j % 2)
            a3[j, o0 * SUB:(o0 + on) * SUB] = tiles
            for p, n in own_rows(b):
                ax[j, p:p + n] = tiles[p - o0 * SUB:p - o0 * SUB + n]
        send_rows(a3, ax, b, js, c3.at[b, g], ssem.at[5], True)

    run = {"pass_on": pass_on, "pass_across": pass_across, "hidden": hidden, "down": down,
           "pair_sum": pair_sum, "answer": answer}
    for name, b, g in plan(len(batches), len(dgroups), len(cgroups)):
        with jax.named_scope(f"{name}_{b}{g}"):
            run[name](b, g)
    for g, (j0, jn) in enumerate(cgroups):
        with jax.named_scope(f"back_{g}"):
            for b, (o0, on) in enumerate(batches):
                arrived(ax.at[pl.ds(j0, jn), pl.ds(o0 * SUB, remote_rows(b))], c3.at[b, g])
        for j in range(j0, j0 + jn):
            answers = from_tiles(ax[j], per, j % 2, 2)
            out_ref[:, j * COLS:(j + 1) * COLS] = jnp.dot(place, answers, preferred_element_type=f32).astype(bf16)
    for i, ref in enumerate((tx.at[:, pl.ds(0, per - SLOT)], rx.at[:, pl.ds(0, nx - 1)], rx.at[:, pl.ds(0, nx)],
                             py.at[:, pl.ds(0, nx)], s2, a3.at[:, pl.ds(0, per - SLOT)])):
        remote(ref, ref, ssem.at[i], ssem.at[i], me_n, partner).wait_send()


def shards(n_node, n_local, tokens, w_gate, w_up, w_down, chosen, counts, gates):
    tok_dev, width = tokens.shape
    ff = w_gate.shape[2]
    chunks = width // COLS
    nx = n_local // 2
    per = n_node * SLOT
    octs = per // SUB
    nb, dg, cg = len(split(octs, BATCHES)), len(split(chunks, DISPATCH_GROUPS)), len(split(chunks, COMBINE_GROUPS))
    deep = max(per, n_local * SUB * split(octs, BATCHES)[0][1])
    bf16 = jnp.bfloat16
    vmem = pl.BlockSpec(memory_space=pltpu.VMEM)
    dma = pltpu.SemaphoreType.DMA
    buffers = [
        ((tok_dev, width), bf16),
        ((width, ff), bf16),
        ((width, ff), bf16),
        ((ff, width), bf16),
        ((chunks, per, SUB, LANE), bf16),
        ((chunks, n_local, per, SUB, LANE), bf16),
        ((chunks, n_local, octs, SUB, COLS), bf16),
        ((chunks, nx, octs, SUB, COLS), bf16),
        ((chunks, nx - 1, octs, SUB, COLS), bf16),
        ((chunks, nx - 1, octs, SUB, COLS), bf16),
        ((chunks, per, SUB, LANE), bf16),
        ((chunks, per, SUB, LANE), bf16),
        ((2, deep * SUB, LANE), jnp.float32),
    ]
    size = sum(functools.reduce(lambda a, b: a * b, shape) * jnp.dtype(kind).itemsize for shape, kind in buffers)
    args = (counts, chosen, gates, tokens, w_gate, w_up, w_down)
    return pl.pallas_call(
        functools.partial(kernel, (n_node, n_local, chunks, tok_dev, ff)),
        out_shape=jax.ShapeDtypeStruct((tok_dev, width), bf16),
        in_specs=[pl.BlockSpec(memory_space=pl.ANY)] * 7,
        out_specs=vmem,
        scratch_shapes=[
            pltpu.SMEM(counts.shape, counts.dtype),
            pltpu.VMEM(chosen.shape, chosen.dtype),
            pltpu.VMEM(gates.shape, gates.dtype),
            *(pltpu.VMEM(shape, kind) for shape, kind in buffers),
            dma((7,)), dma((6,)),
            dma((nb, dg)), dma((nb, dg)), dma((nb, dg)),
            dma((nb, cg)), dma((nb, cg)), dma((nb, cg)),
        ],
        compiler_params=pltpu.CompilerParams(
            collective_id=0, has_side_effects=True, vmem_limit_bytes=min(size + 14000000, 66000000)),
    )(*(pltpu.with_memory_space_constraint(arg, pltpu.HBM) for arg in args))


def solution(mesh):
    in_specs = (
        P(("node", "local"), None),
        P("node", None, "local"),
        P("node", None, "local"),
        P("node", "local", None),
        P(),
        P(),
        P(),
    )
    out_specs = P(("node", "local"), None)
    body = functools.partial(shards, mesh.shape["node"], mesh.shape["local"])
    return jax.shard_map(body, mesh=mesh, in_specs=in_specs, out_specs=out_specs, check_vma=False)
```

```python
import functools

import jax
import jax.numpy as jnp
from jax import lax
from jax.experimental import pallas as pl
from jax.experimental.pallas import tpu as pltpu
from jax.sharding import PartitionSpec as P

SLOT = 3
SUB, LANE = 8, 128
COLS = SUB * LANE
MESH = pl.DeviceIdType.MESH
BATCHES = 3
ACROSS, HOP, NEAR, NEAR_STEP, FAR, FAR_STEP = 2.6, 1.0, 2.2, 0.7, 2.2, 0.75
DISPATCH_GROUPS = 3
COMBINE_GROUPS = 3


def split(count, groups):
    groups = min(groups, count)
    sizes = [count // groups + (1 if g < count % groups else 0) for g in range(groups)]
    starts = [sum(sizes[:g]) for g in range(groups)]
    return list(zip(starts, sizes))


def batches_of(n_node):
    sizes = sorted(count for _, count in split(n_node * SLOT // SUB, BATCHES))
    return [(sum(sizes[:b]), size) for b, size in enumerate(sizes)]


def row_order(n_node):
    far = [(k, s) for k in range(n_node - 1, n_node // 2 - 1, -1) for s in range(SLOT)]
    near = [(k, s) for k in range(n_node // 2 - 1, -1, -1) for s in range(SLOT)]
    rows = []
    for _, octs in batches_of(n_node):
        half = max(octs * SUB // 2, octs * SUB - len(near))
        rows += far[:half] + near[:octs * SUB - half]
        far, near = far[half:], near[octs * SUB - half:]
    return rows


def runs_of(order, first, count):
    runs = []
    for p in range(first, first + count):
        k = order[p][0]
        if runs and runs[-1][0] == k and runs[-1][1] + runs[-1][2] == p:
            runs[-1][2] += 1
        else:
            runs.append([k, p, 1])
    return [tuple(run) for run in runs]


def plan(sizes, dg, cg):
    nb, total = len(sizes), sum(sizes)
    wire = [7.0 * size / total / dg for size in sizes]
    work = {"pass_near": 0.02, "pass_far": 0.02, "pass_across": 0.02, "pair_sum": 0.03, "answer": 0.05,
            "hidden": 1.65 / dg, "down": 1.0 / cg}
    rank = {name: i for i, name in enumerate(("pass_far", "pass_near", "pass_across", "pair_sum", "answer", "hidden", "down"))}
    ready = {}
    passed = 0.0
    for b in range(nb):
        for g in range(dg):
            ready["pass_near", b, g] = NEAR + NEAR_STEP * passed
            passed += 9 * sizes[b] / total / dg
            ready["pass_far", b, g] = FAR + FAR_STEP * passed
    steps, clock, link = [], 0.0, 0.0

    def urgency(step):
        name, b, g = step
        return (b + 4 if name in ("hidden", "down") else 0, rank[name], b, g)

    while ready:
        clock = max(clock, min(ready.values()))
        name, b, g = step = min((s for s in ready if ready[s] <= clock), key=urgency)
        del ready[step]
        steps.append(step)
        clock += work[name]
        if name in ("pass_near", "pass_far"):
            link = max(link, clock) + wire[b] / 2
            if not any(("pass_far" if name == "pass_near" else "pass_near", b, g) == s for s in ready):
                ready["pass_across", b, g] = link + ACROSS
        elif name == "pass_across":
            ready["hidden", b, g] = clock + HOP
        elif name == "hidden":
            if g == dg - 1:
                ready["down", b, 0] = clock
        elif name == "down":
            ready["pair_sum", b, g] = clock + HOP
            if g < cg - 1:
                ready["down", b, g + 1] = clock
        elif name == "pair_sum":
            link = max(link, clock) + wire[b] * dg / cg
            ready["answer", b, g] = link + ACROSS
    return steps


def kernel(dims, counts_hbm, chosen_hbm, gates_hbm, tokens_hbm, wg_hbm, wu_hbm, wd_hbm, out_ref,
           counts_ref, chosen_ref, gates_ref, tokens_ref, wgu, wd, tx, rx, py, r1b, s2, r2b, a3, ax, stage,
           wsem, ssem, d1, d2, d3, c1, c2, c3):
    n_node, n_local, chunks, tok_dev, ff = dims
    nx = n_local // 2
    experts, cap = chosen_ref.shape
    per = n_node * SLOT
    octs = per // SUB
    f32, bf16 = jnp.float32, jnp.bfloat16
    me_n, me_l = lax.axis_index("node"), lax.axis_index("local")
    me_x, me_c = me_l // 2, me_l % 2
    mine, half, other = me_c * nx + me_x, me_c * nx, (1 - me_c) * nx
    partner = me_x * 2 + (1 - me_c)
    order = row_order(n_node)
    batches = batches_of(n_node)
    dgroups, cgroups = split(chunks, DISPATCH_GROUPS), split(chunks, COMBINE_GROUPS)

    paired = n_node & (n_node - 1) == 0

    def node_at(k):
        if paired:
            return jnp.bitwise_xor(me_n, abs(k))
        return lax.rem(me_n + k + n_node, n_node)

    def x_at(k):
        return lax.rem(me_x + k + nx, nx)

    def remote(src, dst, ssem, rsem, node, local):
        return pltpu.make_async_remote_copy(
            src_ref=src, dst_ref=dst, send_sem=ssem, recv_sem=rsem,
            device_id=(node, local), device_id_type=MESH)

    def send(*args):
        remote(*args).start()

    def arrived(ref, sem):
        remote(ref, ref, sem, sem, me_n, partner).wait_recv()

    barrier = pltpu.get_barrier_semaphore()
    for k in range(1, n_node):
        pl.semaphore_signal(barrier, inc=1, device_id=(node_at(k), me_l), device_id_type=MESH)
    pl.semaphore_signal(barrier, inc=1, device_id=(me_n, partner), device_id_type=MESH)
    for k in range(1, nx):
        pl.semaphore_signal(barrier, inc=1, device_id=(me_n, x_at(k) * 2 + me_c), device_id_type=MESH)

    loads = [pltpu.make_async_copy(src, dst, wsem.at[i]) for i, (src, dst) in enumerate((
        (wg_hbm.at[0], wgu.at[:, 0:ff]), (wu_hbm.at[0], wgu.at[:, ff:2 * ff]), (wd_hbm.at[0], wd),
        (counts_hbm, counts_ref), (chosen_hbm, chosen_ref), (gates_hbm, gates_ref),
        *((tokens_hbm.at[:, j0 * COLS:(j0 + jn) * COLS], tokens_ref.at[:, j0 * COLS:(j0 + jn) * COLS]) for j0, jn in dgroups)))]
    for copy in loads[3:]:
        copy.start()
    for copy in loads[3:5]:
        copy.wait()

    base = (me_n * n_local + me_l) * tok_dev
    row = lax.broadcasted_iota(jnp.int32, (experts, cap), 0)
    count = jnp.zeros((experts, cap), jnp.int32)
    for e in range(experts):
        count = jnp.where(row == e, counts_ref[e], count)
    pos = chosen_ref[...] - base
    live = (lax.broadcasted_iota(jnp.int32, (experts, cap), 1) < count) & (pos >= 0) & (pos < tok_dev)
    before = (lax.broadcasted_iota(jnp.int32, (cap, cap), 0)
              < lax.broadcasted_iota(jnp.int32, (cap, cap), 1))
    rank = jnp.dot(jnp.where(live, 1.0, 0.0).astype(bf16), jnp.where(before, 1.0, 0.0).astype(bf16),
                   preferred_element_type=f32)
    pos1 = (pos + 1).astype(f32)
    lane1 = (lax.broadcasted_iota(jnp.int32, (experts, tok_dev), 1) + 1).astype(f32)
    hits = []
    for s in range(SLOT):
        where = jnp.sum(jnp.where(live & (rank == float(s)), pos1, 0.0), axis=1, keepdims=True)
        hits.append(lane1 == where)
    pick = jnp.concatenate([jnp.where(hit, 1.0, 0.0) for hit in hits], axis=0)
    col = lax.broadcasted_iota(jnp.int32, (per, per), 1)
    source = lax.broadcasted_iota(jnp.int32, (per, per), 0)
    wanted = jnp.zeros((per, per), jnp.int32)
    for p, (k, s) in enumerate(order):
        wanted = jnp.where(source == p, node_at(k) + s * experts, wanted)
    permute = jnp.where(col == wanted, 1.0, 0.0).astype(bf16)

    def ordered(x):
        return jnp.dot(permute, x, preferred_element_type=f32)

    select = ordered(pick.astype(bf16)).astype(bf16)

    def to_tiles(value, m, side):
        for q in range(SUB):
            stage[side, pl.ds(q, m, stride=SUB), :] = value[:, q * LANE:(q + 1) * LANE]
        return stage[side, pl.ds(0, m * SUB), :].astype(bf16).reshape(m, SUB, LANE)

    def from_tiles(value, m, side, times=1):
        stage[side, pl.ds(0, m * SUB), :] = value.reshape(m * SUB, LANE).astype(f32)
        parts = [stage[side, pl.ds(q, m, stride=SUB), :] for q in range(SUB)]
        return jnp.concatenate([jnp.concatenate([p] * times, axis=0).astype(bf16) for p in parts], axis=1)

    def runs(b):
        o0, on = batches[b]
        return runs_of(order, o0 * SUB, on * SUB)

    def is_far(k):
        return 2 * k >= n_node

    def part(b, far):
        o0, on = batches[b]
        count = sum(n for k, _, n in runs(b) if is_far(k))
        if far:
            return o0 * SUB, count, sum(n for k, _, n in runs(b) if k and is_far(k))
        return o0 * SUB + count, on * SUB - count, sum(n for k, _, n in runs(b) if k and not is_far(k))

    def remote_rows(b):
        return sum(n for k, _, n in runs(b) if k)

    def own_rows(b):
        return [(p, n) for k, p, n in runs(b) if not k]

    def send_out(b, g):
        js = pl.ds(*dgroups[g])
        for k, p, n in runs(b):
            if k:
                send(tx.at[js, pl.ds(p, n)], rx.at[js, mine, pl.ds(p, n)], ssem.at[0],
                     d1.at[b, g, 1 if is_far(k) else 0], node_at(k), me_l)

    def send_back(b, g):
        js = pl.ds(*cgroups[g])
        for k, p, n in runs(b):
            if k:
                send(a3.at[js, pl.ds(p, n)], ax.at[js, pl.ds(p, n)], ssem.at[5], c3.at[b, g], node_at(-k), me_l)

    for g, (j0, jn) in enumerate(dgroups):
        loads[6 + g].wait()
        for j in range(j0, j0 + jn):
            picked = jnp.dot(select, tokens_ref[:, j * COLS:(j + 1) * COLS], preferred_element_type=f32)
            tiles = to_tiles(picked, per, j % 2)
            tx[j] = tiles
            for b in range(len(batches)):
                for p, n in own_rows(b):
                    rx[j, mine, p:p + n] = tiles[p:p + n]
        if g == 0:
            pl.semaphore_wait(barrier, n_node - 1 + 1 + nx - 1)
        send_out(0, g)
    for copy in loads[:3]:
        copy.start()
    for b in range(1, len(batches)):
        for g in range(len(dgroups)):
            send_out(b, g)

    loads[5].wait()
    weight = jnp.concatenate([
        jnp.where(hits[s], jnp.sum(jnp.where(live & (rank == float(s)), gates_ref[...], 0.0), axis=1, keepdims=True), 0.0)
        for s in range(SLOT)], axis=0)
    high = weight.astype(bf16)
    low = (weight - high.astype(f32)).astype(bf16)
    place = jnp.transpose(jnp.concatenate([ordered(high), ordered(low)], axis=0)).astype(bf16)

    sums, inner = {}, {}

    def pass_part(b, g, far):
        js = pl.ds(*dgroups[g])
        first, count, remotes = part(b, far)
        if remotes:
            arrived(rx.at[js, mine, pl.ds(first, remotes)], d1.at[b, g, 1 if far else 0])
        if count:
            block = rx.at[js, mine, pl.ds(first, count)]
            for d in range(1, nx):
                send(block, block, ssem.at[1], d2.at[b, g], me_n, x_at(d) * 2 + me_c)
            send(block, block, ssem.at[2], d3.at[b, g], me_n, partner)

    def pass_across(b, g):
        o0, on = batches[b]
        js, rows = pl.ds(*dgroups[g]), pl.ds(o0 * SUB, on * SUB)
        arrived(rx.at[js, pl.ds(half, nx - 1), rows], d2.at[b, g])
        for d in range(1, nx):
            block = rx.at[js, half + x_at(-d), rows]
            send(block, block, ssem.at[2], d3.at[b, g], me_n, partner)

    def hidden(b, g):
        o0, on = batches[b]
        j0, jn = dgroups[g]
        m = n_local * on * SUB
        arrived(rx.at[pl.ds(j0, jn), pl.ds(other, nx), pl.ds(o0 * SUB, on * SUB)], d3.at[b, g])
        if b == 0 and g == 0:
            loads[0].wait()
            loads[1].wait()
        x = jnp.concatenate([
            from_tiles(rx[j, :, o0 * SUB:(o0 + on) * SUB].reshape(m, SUB, LANE), m, j % 2)
            for j in range(j0, j0 + jn)], axis=1)
        ks = pl.ds(j0 * COLS, jn * COLS)
        now = jnp.dot(x, wgu[ks, :], preferred_element_type=f32)
        sums[b] = sums[b] + now if b in sums else now
        if g == len(dgroups) - 1:
            gate, up = sums[b][:, 0:ff], sums[b][:, ff:2 * ff]
            inner[b] = (gate / (1.0 + jnp.exp(-gate)) * up).astype(bf16)

    def down(b, g):
        o0, on = batches[b]
        j0, jn = cgroups[g]
        if b == 0 and g == 0:
            loads[2].wait()
        for j in range(j0, j0 + jn):
            y = jnp.dot(inner[b], wd[:, j * COLS:(j + 1) * COLS], preferred_element_type=f32)
            py[j, :, o0:o0 + on] = y.reshape(n_local, on, SUB, COLS).astype(bf16)
        js = pl.ds(j0, jn)
        send(py.at[js, pl.ds(other, nx), pl.ds(o0, on)], r1b.at[js, :, pl.ds(o0, on)],
             ssem.at[3], c1.at[b, g], me_n, partner)

    def pair_sum(b, g):
        o0, on = batches[b]
        j0, jn = cgroups[g]
        js, os = pl.ds(j0, jn), pl.ds(o0, on)
        arrived(r1b.at[js, :, os], c1.at[b, g])
        for d in range(1, nx):
            xd = x_at(d)
            for j in range(j0, j0 + jn):
                s2[j, d - 1, o0:o0 + on] = (py[j, half + xd, o0:o0 + on].astype(f32)
                                            + r1b[j, xd, o0:o0 + on].astype(f32)).astype(bf16)
            send(s2.at[js, d - 1, os], r2b.at[js, d - 1, os], ssem.at[4], c2.at[b, g], me_n, xd * 2 + me_c)

    def answer(b, g):
        o0, on = batches[b]
        j0, jn = cgroups[g]
        js, os = pl.ds(j0, jn), pl.ds(o0, on)
        arrived(r2b.at[js, :, os], c2.at[b, g])
        for j in range(j0, j0 + jn):
            total = py[j, mine, o0:o0 + on].astype(f32) + r1b[j, me_x, o0:o0 + on].astype(f32)
            for d in range(1, nx):
                total = total + r2b[j, d - 1, o0:o0 + on].astype(f32)
            tiles = to_tiles(total.reshape(on * SUB, COLS), on * SUB, j % 2)
            a3[j, o0 * SUB:(o0 + on) * SUB] = tiles
            for p, n in own_rows(b):
                ax[j, p:p + n] = tiles[p - o0 * SUB:p - o0 * SUB + n]
        send_back(b, g)

    run = {"pass_near": functools.partial(pass_part, far=False), "pass_far": functools.partial(pass_part, far=True), "pass_across": pass_across, "hidden": hidden, "down": down,
           "pair_sum": pair_sum, "answer": answer}
    for name, b, g in plan([on for _, on in batches], len(dgroups), len(cgroups)):
        with jax.named_scope(f"{name}_{b}{g}"):
            run[name](b, g)
    for g, (j0, jn) in enumerate(cgroups):
        with jax.named_scope(f"back_{g}"):
            for b, (o0, on) in enumerate(batches):
                arrived(ax.at[pl.ds(j0, jn), pl.ds(o0 * SUB, remote_rows(b))], c3.at[b, g])
        for j in range(j0, j0 + jn):
            answers = from_tiles(ax[j], per, j % 2, 2)
            out_ref[:, j * COLS:(j + 1) * COLS] = jnp.dot(place, answers, preferred_element_type=f32).astype(bf16)
    for i, ref in enumerate((tx.at[:, pl.ds(0, per - SLOT)], rx.at[:, pl.ds(0, nx - 1)], rx.at[:, pl.ds(0, nx)],
                             py.at[:, pl.ds(0, nx)], s2, a3.at[:, pl.ds(0, per - SLOT)])):
        remote(ref, ref, ssem.at[i], ssem.at[i], me_n, partner).wait_send()


def shards(n_node, n_local, tokens, w_gate, w_up, w_down, chosen, counts, gates):
    tok_dev, width = tokens.shape
    ff = w_gate.shape[2]
    chunks = width // COLS
    nx = n_local // 2
    per = n_node * SLOT
    octs = per // SUB
    nb, dg, cg = len(split(octs, BATCHES)), len(split(chunks, DISPATCH_GROUPS)), len(split(chunks, COMBINE_GROUPS))
    deep = max(per, n_local * SUB * batches_of(n_node)[-1][1])
    bf16 = jnp.bfloat16
    vmem = pl.BlockSpec(memory_space=pltpu.VMEM)
    dma = pltpu.SemaphoreType.DMA
    buffers = [
        ((tok_dev, width), bf16),
        ((width, 2 * ff), bf16),
        ((ff, width), bf16),
        ((chunks, per, SUB, LANE), bf16),
        ((chunks, n_local, per, SUB, LANE), bf16),
        ((chunks, n_local, octs, SUB, COLS), bf16),
        ((chunks, nx, octs, SUB, COLS), bf16),
        ((chunks, nx - 1, octs, SUB, COLS), bf16),
        ((chunks, nx - 1, octs, SUB, COLS), bf16),
        ((chunks, per, SUB, LANE), bf16),
        ((chunks, per, SUB, LANE), bf16),
        ((2, deep * SUB, LANE), jnp.float32),
    ]
    size = sum(functools.reduce(lambda a, b: a * b, shape) * jnp.dtype(kind).itemsize for shape, kind in buffers)
    args = (counts, chosen, gates, tokens, w_gate, w_up, w_down)
    return pl.pallas_call(
        functools.partial(kernel, (n_node, n_local, chunks, tok_dev, ff)),
        out_shape=jax.ShapeDtypeStruct((tok_dev, width), bf16),
        in_specs=[pl.BlockSpec(memory_space=pl.ANY)] * 7,
        out_specs=vmem,
        scratch_shapes=[
            pltpu.SMEM(counts.shape, counts.dtype),
            pltpu.VMEM(chosen.shape, chosen.dtype),
            pltpu.VMEM(gates.shape, gates.dtype),
            *(pltpu.VMEM(shape, kind) for shape, kind in buffers),
            dma((6 + dg,)), dma((6,)),
            dma((nb, dg, 2)), dma((nb, dg)), dma((nb, dg)),
            dma((nb, cg)), dma((nb, cg)), dma((nb, cg)),
        ],
        compiler_params=pltpu.CompilerParams(
            collective_id=0, has_side_effects=True, vmem_limit_bytes=min(size + 14000000, 66000000)),
    )(*(pltpu.with_memory_space_constraint(arg, pltpu.HBM) for arg in args))


def solution(mesh):
    in_specs = (
        P(("node", "local"), None),
        P("node", None, "local"),
        P("node", None, "local"),
        P("node", "local", None),
        P(),
        P(),
        P(),
    )
    out_specs = P(("node", "local"), None)
    body = functools.partial(shards, mesh.shape["node"], mesh.shape["local"])
    return jax.shard_map(body, mesh=mesh, in_specs=in_specs, out_specs=out_specs, check_vma=False)
```

```python
import functools

import jax
import jax.numpy as jnp
from jax import lax
from jax.experimental import pallas as pl
from jax.experimental.pallas import tpu as pltpu
from jax.sharding import PartitionSpec as P

SLOT = 3
SUB, LANE = 8, 128
COLS = SUB * LANE
MESH = pl.DeviceIdType.MESH
BATCHES = 3
ACROSS, HOP, NEAR, NEAR_STEP, FAR, FAR_STEP = 2.6, 1.0, 2.6, 0.9, 2.2, 0.9
EARLY = 2
GROUPS = 3


def split(count, groups):
    groups = min(groups, count)
    sizes = [count // groups + (1 if g < count % groups else 0) for g in range(groups)]
    starts = [sum(sizes[:g]) for g in range(groups)]
    return list(zip(starts, sizes))


def batches_of(n_node):
    sizes = sorted(count for _, count in split(n_node * SLOT // SUB, BATCHES))
    return [(sum(sizes[:b]), size) for b, size in enumerate(sizes)]


def row_order(n_node):
    far = [(k, s) for k in range(n_node - 1, n_node // 2 - 1, -1) for s in range(SLOT)]
    near = [(k, s) for k in range(n_node // 2 - 1, -1, -1) for s in range(SLOT)]
    rows = []
    for _, octs in batches_of(n_node):
        half = max(octs * SUB // 2, octs * SUB - len(near))
        rows += far[:half] + near[:octs * SUB - half]
        far, near = far[half:], near[octs * SUB - half:]
    return rows


def runs_of(order, first, count):
    runs = []
    for p in range(first, first + count):
        k = order[p][0]
        if runs and runs[-1][0] == k and runs[-1][1] + runs[-1][2] == p:
            runs[-1][2] += 1
        else:
            runs.append([k, p, 1])
    return [tuple(run) for run in runs]


def plan(sizes, ng):
    nb, total = len(sizes), sum(sizes)
    wire = [7.0 * size / total / ng for size in sizes]
    work = {"pass_near": 0.02, "pass_far": 0.02, "pass_across": 0.02, "pair_sum": 0.03, "answer": 0.05,
            "hidden": 1.65 / ng, "down": 1.0 / ng}
    rank = {name: i for i, name in enumerate(("pass_far", "pass_near", "pass_across", "pair_sum", "answer", "hidden", "down"))}
    ready = {}
    passed = 0.0
    for b in range(nb):
        for g in range(ng):
            ready["pass_near", b, g] = NEAR + NEAR_STEP * passed
            passed += 9 * sizes[b] / total / ng
            ready["pass_far", b, g] = FAR + FAR_STEP * passed
    steps, clock, link = [], 0.0, 0.0

    def urgency(step):
        name, b, g = step
        return (b + 4 if name in ("hidden", "down") else 0, rank[name], b, g)

    while ready:
        clock = max(clock, min(ready.values()))
        name, b, g = step = min((s for s in ready if ready[s] <= clock), key=urgency)
        del ready[step]
        steps.append(step)
        clock += work[name] * ((0.55, 1.5, 0.95)[min(g, 2)] if name == "hidden" and ng == 3 else 1.0)
        if name in ("pass_near", "pass_far"):
            link = max(link, clock) + wire[b] / 2
            if not any(("pass_far" if name == "pass_near" else "pass_near", b, g) == s for s in ready):
                ready["pass_across", b, g] = link + ACROSS
        elif name == "pass_across":
            ready["hidden", b, g] = clock + HOP
        elif name == "hidden":
            if g == ng - 1:
                ready["down", b, 0] = clock
        elif name == "down":
            ready["pair_sum", b, g] = clock + HOP
            if g < ng - 1:
                ready["down", b, g + 1] = clock
        elif name == "pair_sum":
            link = max(link, clock) + wire[b]
            ready["answer", b, g] = link + ACROSS
    return steps


def kernel(dims, counts_hbm, chosen_hbm, gates_hbm, tokens_hbm, wg_hbm, wu_hbm, wd_hbm, out_ref,
           counts_ref, chosen_ref, gates_ref, tokens_ref, wgu, wd, tx, rx, py, r1b, s2, r2b, a3, ax, stage,
           wsem, psem, ssem, d1, d2, d3, c3):
    n_node, n_local, chunks, tok_dev, ff = dims
    nx = n_local // 2
    experts, cap = chosen_ref.shape
    per = n_node * SLOT
    octs = per // SUB
    f32, bf16 = jnp.float32, jnp.bfloat16
    me_n, me_l = lax.axis_index("node"), lax.axis_index("local")
    me_x, me_c = me_l // 2, me_l % 2
    mine, half, other = me_c * nx + me_x, me_c * nx, (1 - me_c) * nx
    partner = me_x * 2 + (1 - me_c)
    order = row_order(n_node)
    batches = batches_of(n_node)
    groups = split(chunks, GROUPS)

    paired = n_node & (n_node - 1) == 0

    def node_at(k):
        if paired:
            return jnp.bitwise_xor(me_n, abs(k))
        return lax.rem(me_n + k + n_node, n_node)

    def x_at(k):
        return lax.rem(me_x + k + nx, nx)

    def remote(src, dst, ssem, rsem, node, local):
        return pltpu.make_async_remote_copy(
            src_ref=src, dst_ref=dst, send_sem=ssem, recv_sem=rsem,
            device_id=(node, local), device_id_type=MESH)

    def send(*args):
        remote(*args).start()

    def arrived(ref, sem):
        remote(ref, ref, sem, sem, me_n, partner).wait_recv()

    barrier = pltpu.get_barrier_semaphore()
    for k in range(1, n_node):
        pl.semaphore_signal(barrier, inc=1, device_id=(node_at(k), me_l), device_id_type=MESH)
    pl.semaphore_signal(barrier, inc=1, device_id=(me_n, partner), device_id_type=MESH)
    for k in range(1, nx):
        pl.semaphore_signal(barrier, inc=1, device_id=(me_n, x_at(k) * 2 + me_c), device_id_type=MESH)

    loads = [pltpu.make_async_copy(src, dst, wsem.at[i]) for i, (src, dst) in enumerate((
        (wd_hbm.at[0], wd), (counts_hbm, counts_ref), (chosen_hbm, chosen_ref), (gates_hbm, gates_ref),
        *((tokens_hbm.at[:, j0 * COLS:(j0 + jn) * COLS], tokens_ref.at[:, j0 * COLS:(j0 + jn) * COLS]) for j0, jn in groups)))]
    panels = [pltpu.make_async_copy(src.at[0, :, i * LANE:(i + 1) * LANE], wgu.at[which * (ff // LANE) + i], psem.at[0])
              for which, src in enumerate((wg_hbm, wu_hbm)) for i in range(ff // LANE)]
    for copy in loads[1:]:
        copy.start()
    for copy in loads[1:3]:
        copy.wait()

    base = (me_n * n_local + me_l) * tok_dev
    row = lax.broadcasted_iota(jnp.int32, (experts, cap), 0)
    count = jnp.zeros((experts, cap), jnp.int32)
    for e in range(experts):
        count = jnp.where(row == e, counts_ref[e], count)
    pos = chosen_ref[...] - base
    live = (lax.broadcasted_iota(jnp.int32, (experts, cap), 1) < count) & (pos >= 0) & (pos < tok_dev)
    before = (lax.broadcasted_iota(jnp.int32, (cap, cap), 0)
              < lax.broadcasted_iota(jnp.int32, (cap, cap), 1))
    rank = jnp.dot(jnp.where(live, 1.0, 0.0).astype(bf16), jnp.where(before, 1.0, 0.0).astype(bf16),
                   preferred_element_type=f32)
    pos1 = (pos + 1).astype(f32)
    lane1 = (lax.broadcasted_iota(jnp.int32, (experts, tok_dev), 1) + 1).astype(f32)
    hits = []
    for s in range(SLOT):
        where = jnp.sum(jnp.where(live & (rank == float(s)), pos1, 0.0), axis=1, keepdims=True)
        hits.append(lane1 == where)
    pick = jnp.concatenate([jnp.where(hit, 1.0, 0.0) for hit in hits], axis=0)
    col = lax.broadcasted_iota(jnp.int32, (per, per), 1)
    source = lax.broadcasted_iota(jnp.int32, (per, per), 0)
    wanted = jnp.zeros((per, per), jnp.int32)
    for p, (k, s) in enumerate(order):
        wanted = jnp.where(source == p, node_at(k) + s * experts, wanted)
    permute = jnp.where(col == wanted, 1.0, 0.0).astype(bf16)

    def ordered(x):
        return jnp.dot(permute, x, preferred_element_type=f32)

    select = ordered(pick.astype(bf16)).astype(bf16)

    def to_tiles(value, m, side):
        for q in range(SUB):
            stage[side, pl.ds(q, m, stride=SUB), :] = value[:, q * LANE:(q + 1) * LANE]
        return stage[side, pl.ds(0, m * SUB), :].astype(bf16).reshape(m, SUB, LANE)

    def from_tiles(value, m, side, times=1):
        stage[side, pl.ds(0, m * SUB), :] = value.reshape(m * SUB, LANE).astype(f32)
        parts = [stage[side, pl.ds(q, m, stride=SUB), :] for q in range(SUB)]
        return jnp.concatenate([jnp.concatenate([p] * times, axis=0).astype(bf16) for p in parts], axis=1)

    def runs(b):
        o0, on = batches[b]
        return runs_of(order, o0 * SUB, on * SUB)

    def is_far(k):
        return 2 * k >= n_node

    def part(b, far):
        o0, on = batches[b]
        count = sum(n for k, _, n in runs(b) if is_far(k))
        if far:
            return o0 * SUB, count, sum(n for k, _, n in runs(b) if k and is_far(k))
        return o0 * SUB + count, on * SUB - count, sum(n for k, _, n in runs(b) if k and not is_far(k))

    def own_rows(b):
        return [(p, n) for k, p, n in runs(b) if not k]

    def send_out(b, g):
        js = pl.ds(*groups[g])
        for k, p, n in runs(b):
            if k:
                send(tx.at[js, pl.ds(p, n)], rx.at[js, mine, pl.ds(p, n)], ssem.at[0],
                     d1.at[b, g, 1 if is_far(k) else 0], node_at(k), me_l)

    def send_back(b, g):
        js = pl.ds(*groups[g])
        for k, p, n in runs(b):
            if k:
                send(a3.at[js, pl.ds(p, n)], ax.at[js, pl.ds(p, n)], ssem.at[5], c3.at[g], node_at(-k), me_l)

    for g, (j0, jn) in enumerate(groups):
        loads[4 + g].wait()
        for j in range(j0, j0 + jn):
            picked = jnp.dot(select, tokens_ref[:, j * COLS:(j + 1) * COLS], preferred_element_type=f32)
            tiles = to_tiles(picked, per, j % 2)
            tx[j] = tiles
            for b in range(len(batches)):
                for p, n in own_rows(b):
                    rx[j, mine, p:p + n] = tiles[p:p + n]
        if g == 0:
            pl.semaphore_wait(barrier, n_node - 1 + 1 + nx - 1)
        send_out(0, g)
    for copy in [*panels, loads[0]]:
        copy.start()
    for b in range(1, min(EARLY, len(batches))):
        for g in range(len(groups)):
            send_out(b, g)

    loads[3].wait()
    weight = jnp.concatenate([
        jnp.where(hits[s], jnp.sum(jnp.where(live & (rank == float(s)), gates_ref[...], 0.0), axis=1, keepdims=True), 0.0)
        for s in range(SLOT)], axis=0)
    high = weight.astype(bf16)
    low = (weight - high.astype(f32)).astype(bf16)
    place = jnp.transpose(jnp.concatenate([ordered(high), ordered(low)], axis=0)).astype(bf16)

    sums, inner = {}, {}

    def pass_part(b, g, far):
        js = pl.ds(*groups[g])
        first, count, remotes = part(b, far)
        if remotes:
            arrived(rx.at[js, mine, pl.ds(first, remotes)], d1.at[b, g, 1 if far else 0])
        if count:
            block = rx.at[js, mine, pl.ds(first, count)]
            for d in range(1, nx):
                send(block, block, ssem.at[1], d2.at[b, g], me_n, x_at(d) * 2 + me_c)
            send(block, block, ssem.at[2], d3.at[b, g], me_n, partner)

    def pass_across(b, g):
        o0, on = batches[b]
        js, rows = pl.ds(*groups[g]), pl.ds(o0 * SUB, on * SUB)
        arrived(rx.at[js, pl.ds(half, nx - 1), rows], d2.at[b, g])
        for d in range(1, nx):
            block = rx.at[js, half + x_at(-d), rows]
            send(block, block, ssem.at[2], d3.at[b, g], me_n, partner)

    def hidden(b, g):
        o0, on = batches[b]
        j0, jn = groups[g]
        m = n_local * on * SUB
        arrived(rx.at[pl.ds(j0, jn), pl.ds(other, nx), pl.ds(o0 * SUB, on * SUB)], d3.at[b, g])
        if b == 0 and g == 0:
            pltpu.make_async_copy(wgu, wgu, psem.at[0]).wait()
        x = jnp.concatenate([
            from_tiles(rx[j, :, o0 * SUB:(o0 + on) * SUB].reshape(m, SUB, LANE), m, j % 2)
            for j in range(j0, j0 + jn)], axis=1)
        ks = pl.ds(j0 * COLS, jn * COLS)
        both = jnp.concatenate([wgu[i, ks, :] for i in range(2 * ff // LANE)], axis=1)
        now = jnp.dot(x, both, preferred_element_type=f32)
        sums[b] = sums[b] + now if b in sums else now
        if g == len(groups) - 1:
            gate, up = sums[b][:, 0:ff], sums[b][:, ff:2 * ff]
            inner[b] = (gate / (1.0 + jnp.exp(-gate)) * up).astype(bf16)

    def down(b, g):
        o0, on = batches[b]
        j0, jn = groups[g]
        if b == 0 and g == 0:
            loads[0].wait()
        for j in range(j0, j0 + jn):
            y = jnp.dot(inner[b], wd[:, j * COLS:(j + 1) * COLS], preferred_element_type=f32)
            py[j, :, o0:o0 + on] = y.reshape(n_local, on, SUB, COLS).astype(bf16)
        js = pl.ds(j0, jn)
        send(py.at[js, pl.ds(other, nx), pl.ds(o0, on)], r1b.at[js, :, pl.ds(o0, on)],
             ssem.at[3], d1.at[b, g, 0], me_n, partner)

    def pair_sum(b, g):
        o0, on = batches[b]
        j0, jn = groups[g]
        js, os = pl.ds(j0, jn), pl.ds(o0, on)
        arrived(r1b.at[js, :, os], d1.at[b, g, 0])
        for d in range(1, nx):
            xd = x_at(d)
            for j in range(j0, j0 + jn):
                s2[j, d - 1, o0:o0 + on] = (py[j, half + xd, o0:o0 + on].astype(f32)
                                            + r1b[j, xd, o0:o0 + on].astype(f32)).astype(bf16)
            send(s2.at[js, d - 1, os], r2b.at[js, d - 1, os], ssem.at[4], d1.at[b, g, 1], me_n, xd * 2 + me_c)

    def answer(b, g):
        o0, on = batches[b]
        j0, jn = groups[g]
        js, os = pl.ds(j0, jn), pl.ds(o0, on)
        arrived(r2b.at[js, :, os], d1.at[b, g, 1])
        for j in range(j0, j0 + jn):
            total = py[j, mine, o0:o0 + on].astype(f32) + r1b[j, me_x, o0:o0 + on].astype(f32)
            for d in range(1, nx):
                total = total + r2b[j, d - 1, o0:o0 + on].astype(f32)
            tiles = to_tiles(total.reshape(on * SUB, COLS), on * SUB, j % 2)
            a3[j, o0 * SUB:(o0 + on) * SUB] = tiles
            for p, n in own_rows(b):
                ax[j, p:p + n] = tiles[p - o0 * SUB:p - o0 * SUB + n]
        send_back(b, g)

    run = {"pass_near": functools.partial(pass_part, far=False), "pass_far": functools.partial(pass_part, far=True), "pass_across": pass_across, "hidden": hidden, "down": down,
           "pair_sum": pair_sum, "answer": answer}
    for name, b, g in plan([on for _, on in batches], len(groups)):
        with jax.named_scope(f"{name}_{b}{g}"):
            run[name](b, g)
        if (name, b, g) == ("pass_far", 0, len(groups) - 1):
            for late in range(EARLY, len(batches)):
                for i in range(len(groups)):
                    send_out(late, i)
    for g, (j0, jn) in enumerate(groups):
        with jax.named_scope(f"back_{g}"):
            arrived(ax.at[pl.ds(j0, jn), pl.ds(0, per - SLOT)], c3.at[g])
        for j in range(j0, j0 + jn):
            answers = from_tiles(ax[j], per, j % 2, 2)
            out_ref[:, j * COLS:(j + 1) * COLS] = jnp.dot(place, answers, preferred_element_type=f32).astype(bf16)
    for i, ref in enumerate((tx.at[:, pl.ds(0, per - SLOT)], rx.at[:, pl.ds(0, nx - 1)], rx.at[:, pl.ds(0, nx)],
                             py.at[:, pl.ds(0, nx)], s2, a3.at[:, pl.ds(0, per - SLOT)])):
        remote(ref, ref, ssem.at[i], ssem.at[i], me_n, partner).wait_send()


def shards(n_node, n_local, tokens, w_gate, w_up, w_down, chosen, counts, gates):
    tok_dev, width = tokens.shape
    ff = w_gate.shape[2]
    chunks = width // COLS
    nx = n_local // 2
    per = n_node * SLOT
    octs = per // SUB
    nb, ng = len(batches_of(n_node)), len(split(chunks, GROUPS))
    deep = max(per, n_local * SUB * batches_of(n_node)[-1][1])
    bf16 = jnp.bfloat16
    vmem = pl.BlockSpec(memory_space=pltpu.VMEM)
    dma = pltpu.SemaphoreType.DMA
    buffers = [
        ((tok_dev, width), bf16),
        ((2 * ff // LANE, width, LANE), bf16),
        ((ff, width), bf16),
        ((chunks, per, SUB, LANE), bf16),
        ((chunks, n_local, per, SUB, LANE), bf16),
        ((chunks, n_local, octs, SUB, COLS), bf16),
        ((chunks, nx, octs, SUB, COLS), bf16),
        ((chunks, nx - 1, octs, SUB, COLS), bf16),
        ((chunks, nx - 1, octs, SUB, COLS), bf16),
        ((chunks, per, SUB, LANE), bf16),
        ((chunks, per, SUB, LANE), bf16),
        ((2, deep * SUB, LANE), jnp.float32),
    ]
    size = sum(functools.reduce(lambda a, b: a * b, shape) * jnp.dtype(kind).itemsize for shape, kind in buffers)
    args = (counts, chosen, gates, tokens, w_gate, w_up, w_down)
    return pl.pallas_call(
        functools.partial(kernel, (n_node, n_local, chunks, tok_dev, ff)),
        out_shape=jax.ShapeDtypeStruct((tok_dev, width), bf16),
        in_specs=[pl.BlockSpec(memory_space=pl.ANY)] * 7,
        out_specs=vmem,
        scratch_shapes=[
            pltpu.SMEM(counts.shape, counts.dtype),
            pltpu.VMEM(chosen.shape, chosen.dtype),
            pltpu.VMEM(gates.shape, gates.dtype),
            *(pltpu.VMEM(shape, kind) for shape, kind in buffers),
            dma((4 + ng,)), dma((1,)), dma((6,)),
            dma((nb, ng, 2)), dma((nb, ng)), dma((nb, ng)), dma((ng,)),
        ],
        compiler_params=pltpu.CompilerParams(
            collective_id=0, has_side_effects=True, vmem_limit_bytes=min(size + 14000000, 66000000)),
    )(*(pltpu.with_memory_space_constraint(arg, pltpu.HBM) for arg in args))


def solution(mesh):
    in_specs = (
        P(("node", "local"), None),
        P("node", None, "local"),
        P("node", None, "local"),
        P("node", "local", None),
        P(),
        P(),
        P(),
    )
    out_specs = P(("node", "local"), None)
    body = functools.partial(shards, mesh.shape["node"], mesh.shape["local"])
    return jax.shard_map(body, mesh=mesh, in_specs=in_specs, out_specs=out_specs, check_vma=False)
```

```python
import functools

import jax
import jax.numpy as jnp
from jax import lax
from jax.experimental import pallas as pl
from jax.experimental.pallas import tpu as pltpu
from jax.sharding import PartitionSpec as P

SLOT = 3
SUB, LANE = 8, 128
COLS = SUB * LANE
MESH = pl.DeviceIdType.MESH
BATCHES = 3
ACROSS, HOP, NEAR, NEAR_STEP, FAR, FAR_STEP = 2.6, 1.0, 2.6, 0.9, 2.2, 0.9
EARLY = 2
GROUPS = 3


def split(count, groups):
    groups = min(groups, count)
    sizes = [count // groups + (1 if g < count % groups else 0) for g in range(groups)]
    starts = [sum(sizes[:g]) for g in range(groups)]
    return list(zip(starts, sizes))


def batches_of(n_node):
    sizes = sorted(count for _, count in split(n_node * SLOT // SUB, BATCHES))
    return [(sum(sizes[:b]), size) for b, size in enumerate(sizes)]


def row_order(n_node):
    far = [(k, s) for k in range(n_node - 1, n_node // 2 - 1, -1) for s in range(SLOT)]
    near = [(k, s) for k in range(n_node // 2 - 1, -1, -1) for s in range(SLOT)]
    rows = []
    for _, octs in batches_of(n_node):
        half = max(octs * SUB // 2, octs * SUB - len(near))
        rows += far[:half] + near[:octs * SUB - half]
        far, near = far[half:], near[octs * SUB - half:]
    return rows


def runs_of(order, first, count):
    runs = []
    for p in range(first, first + count):
        k = order[p][0]
        if runs and runs[-1][0] == k and runs[-1][1] + runs[-1][2] == p:
            runs[-1][2] += 1
        else:
            runs.append([k, p, 1])
    return [tuple(run) for run in runs]


def plan(sizes, ng):
    nb, total = len(sizes), sum(sizes)
    wire = [7.0 * size / total / ng for size in sizes]
    work = {"pass_near": 0.02, "pass_far": 0.02, "pass_across": 0.02, "pair_sum": 0.03, "answer": 0.05,
            "hidden": 1.65 / ng, "down": 1.0 / ng}
    rank = {name: i for i, name in enumerate(("pair_sum", "pass_far", "pass_near", "pass_across", "answer", "hidden", "down"))}
    ready = {}
    passed = 0.0
    for b in range(nb):
        for g in range(ng):
            ready["pass_near", b, g] = NEAR + NEAR_STEP * passed
            passed += 9 * sizes[b] / total / ng
            ready["pass_far", b, g] = FAR + FAR_STEP * passed
    steps, clock, link = [], 0.0, 0.0

    def urgency(step):
        name, b, g = step
        return (b + 4 if name in ("hidden", "down") else 0, rank[name], b, g)

    while ready:
        clock = max(clock, min(ready.values()))
        name, b, g = step = min((s for s in ready if ready[s] <= clock), key=urgency)
        del ready[step]
        steps.append(step)
        clock += work[name] * ((0.55, 1.5, 0.95)[min(g, 2)] if name == "hidden" and ng == 3 else 1.0)
        if name in ("pass_near", "pass_far"):
            link = max(link, clock) + wire[b] / 2
            if not any(("pass_far" if name == "pass_near" else "pass_near", b, g) == s for s in ready):
                ready["pass_across", b, g] = link + ACROSS
        elif name == "pass_across":
            ready["hidden", b, g] = clock + HOP
        elif name == "hidden":
            if g == ng - 1:
                ready["down", b, 0] = clock
        elif name == "down":
            ready["pair_sum", b, g] = clock + HOP
            if g < ng - 1:
                ready["down", b, g + 1] = clock
        elif name == "pair_sum":
            link = max(link, clock) + wire[b]
            ready["answer", b, g] = link + ACROSS
    return steps


def kernel(dims, counts_hbm, chosen_hbm, gates_hbm, tokens_hbm, wg_hbm, wu_hbm, wd_hbm, out_ref,
           counts_ref, chosen_ref, gates_ref, tokens_ref, wgu, wd, tx, rx, py, r1b, s2, r2b, a3, ax, stage,
           wsem, psem, ssem, d1, d2, d3, c3):
    n_node, n_local, chunks, tok_dev, ff = dims
    nx = n_local // 2
    experts, cap = chosen_ref.shape
    per = n_node * SLOT
    octs = per // SUB
    f32, bf16 = jnp.float32, jnp.bfloat16
    me_n, me_l = lax.axis_index("node"), lax.axis_index("local")
    me_x, me_c = me_l // 2, me_l % 2
    mine, half, other = me_c * nx + me_x, me_c * nx, (1 - me_c) * nx
    partner = me_x * 2 + (1 - me_c)
    order = row_order(n_node)
    batches = batches_of(n_node)
    groups = split(chunks, GROUPS)

    paired = n_node & (n_node - 1) == 0

    def node_at(k):
        if paired:
            return jnp.bitwise_xor(me_n, abs(k))
        return lax.rem(me_n + k + n_node, n_node)

    def x_at(k):
        return lax.rem(me_x + k + nx, nx)

    def remote(src, dst, ssem, rsem, node, local):
        return pltpu.make_async_remote_copy(
            src_ref=src, dst_ref=dst, send_sem=ssem, recv_sem=rsem,
            device_id=(node, local), device_id_type=MESH)

    def send(*args):
        remote(*args).start()

    def arrived(ref, sem):
        remote(ref, ref, sem, sem, me_n, partner).wait_recv()

    barrier = pltpu.get_barrier_semaphore()
    for k in range(1, n_node):
        pl.semaphore_signal(barrier, inc=1, device_id=(node_at(k), me_l), device_id_type=MESH)
    pl.semaphore_signal(barrier, inc=1, device_id=(me_n, partner), device_id_type=MESH)
    for k in range(1, nx):
        pl.semaphore_signal(barrier, inc=1, device_id=(me_n, x_at(k) * 2 + me_c), device_id_type=MESH)

    loads = [pltpu.make_async_copy(src, dst, wsem.at[i]) for i, (src, dst) in enumerate((
        (wd_hbm.at[0], wd), (counts_hbm, counts_ref), (chosen_hbm, chosen_ref), (gates_hbm, gates_ref),
        *((tokens_hbm.at[:, j0 * COLS:(j0 + jn) * COLS], tokens_ref.at[:, j0 * COLS:(j0 + jn) * COLS]) for j0, jn in groups)))]
    panels = [pltpu.make_async_copy(src.at[0, :, i * LANE:(i + 1) * LANE], wgu.at[which * (ff // LANE) + i], psem.at[0])
              for which, src in enumerate((wg_hbm, wu_hbm)) for i in range(ff // LANE)]
    for copy in loads[1:]:
        copy.start()
    for copy in loads[1:3]:
        copy.wait()

    base = (me_n * n_local + me_l) * tok_dev
    row = lax.broadcasted_iota(jnp.int32, (experts, cap), 0)
    count = jnp.zeros((experts, cap), jnp.int32)
    for e in range(experts):
        count = jnp.where(row == e, counts_ref[e], count)
    pos = chosen_ref[...] - base
    live = (lax.broadcasted_iota(jnp.int32, (experts, cap), 1) < count) & (pos >= 0) & (pos < tok_dev)
    before = (lax.broadcasted_iota(jnp.int32, (cap, cap), 0)
              < lax.broadcasted_iota(jnp.int32, (cap, cap), 1))
    rank = jnp.dot(jnp.where(live, 1.0, 0.0).astype(bf16), jnp.where(before, 1.0, 0.0).astype(bf16),
                   preferred_element_type=f32)
    pos1 = (pos + 1).astype(f32)
    lane1 = (lax.broadcasted_iota(jnp.int32, (experts, tok_dev), 1) + 1).astype(f32)
    hits = []
    for s in range(SLOT):
        where = jnp.sum(jnp.where(live & (rank == float(s)), pos1, 0.0), axis=1, keepdims=True)
        hits.append(lane1 == where)
    pick = jnp.concatenate([jnp.where(hit, 1.0, 0.0) for hit in hits], axis=0)
    col = lax.broadcasted_iota(jnp.int32, (per, per), 1)
    source = lax.broadcasted_iota(jnp.int32, (per, per), 0)
    wanted = jnp.zeros((per, per), jnp.int32)
    for p, (k, s) in enumerate(order):
        wanted = jnp.where(source == p, node_at(k) + s * experts, wanted)
    permute = jnp.where(col == wanted, 1.0, 0.0).astype(bf16)

    def ordered(x):
        return jnp.dot(permute, x, preferred_element_type=f32)

    select = ordered(pick.astype(bf16)).astype(bf16)

    def to_tiles(value, m, side):
        for q in range(SUB):
            stage[side, pl.ds(q, m, stride=SUB), :] = value[:, q * LANE:(q + 1) * LANE]
        return stage[side, pl.ds(0, m * SUB), :].astype(bf16).reshape(m, SUB, LANE)

    def from_tiles(value, m, side, times=1):
        stage[side, pl.ds(0, m * SUB), :] = value.reshape(m * SUB, LANE).astype(f32)
        parts = [stage[side, pl.ds(q, m, stride=SUB), :] for q in range(SUB)]
        return jnp.concatenate([jnp.concatenate([p] * times, axis=0).astype(bf16) for p in parts], axis=1)

    def runs(b):
        o0, on = batches[b]
        return runs_of(order, o0 * SUB, on * SUB)

    def is_far(k):
        return 2 * k >= n_node

    def part(b, far):
        o0, on = batches[b]
        count = sum(n for k, _, n in runs(b) if is_far(k))
        if far:
            return o0 * SUB, count, sum(n for k, _, n in runs(b) if k and is_far(k))
        return o0 * SUB + count, on * SUB - count, sum(n for k, _, n in runs(b) if k and not is_far(k))

    def own_rows(b):
        return [(p, n) for k, p, n in runs(b) if not k]

    def send_out(b, g):
        js = pl.ds(*groups[g])
        for k, p, n in runs(b):
            if k:
                send(tx.at[js, pl.ds(p, n)], rx.at[js, mine, pl.ds(p, n)], ssem.at[0],
                     d1.at[b, g, 1 if is_far(k) else 0], node_at(k), me_l)

    def send_back(b, g):
        js = pl.ds(*groups[g])
        for k, p, n in runs(b):
            if k:
                send(a3.at[js, pl.ds(p, n)], ax.at[js, pl.ds(p, n)], ssem.at[5], c3.at[g], node_at(-k), me_l)

    for g, (j0, jn) in enumerate(groups):
        loads[4 + g].wait()
        for j in range(j0, j0 + jn):
            picked = jnp.dot(select, tokens_ref[:, j * COLS:(j + 1) * COLS], preferred_element_type=f32)
            tiles = to_tiles(picked, per, j % 2)
            tx[j] = tiles
            for b in range(len(batches)):
                for p, n in own_rows(b):
                    rx[j, mine, p:p + n] = tiles[p:p + n]
        if g == 0:
            pl.semaphore_wait(barrier, n_node - 1 + 1 + nx - 1)
        send_out(0, g)
    for copy in [*panels, loads[0]]:
        copy.start()
    for b in range(1, min(EARLY, len(batches))):
        for g in range(len(groups)):
            send_out(b, g)

    loads[3].wait()
    weight = jnp.concatenate([
        jnp.where(hits[s], jnp.sum(jnp.where(live & (rank == float(s)), gates_ref[...], 0.0), axis=1, keepdims=True), 0.0)
        for s in range(SLOT)], axis=0)
    high = weight.astype(bf16)
    low = (weight - high.astype(f32)).astype(bf16)
    place = jnp.transpose(jnp.concatenate([ordered(high), ordered(low)], axis=0)).astype(bf16)

    sums, inner = {}, {}

    def pass_part(b, g, far):
        js = pl.ds(*groups[g])
        first, count, remotes = part(b, far)
        if remotes:
            arrived(rx.at[js, mine, pl.ds(first, remotes)], d1.at[b, g, 1 if far else 0])
        if count:
            block = rx.at[js, mine, pl.ds(first, count)]
            for d in range(1, nx):
                send(block, block, ssem.at[1], d2.at[b, g], me_n, x_at(d) * 2 + me_c)
            send(block, block, ssem.at[2], d3.at[b, g], me_n, partner)

    def pass_across(b, g):
        o0, on = batches[b]
        js, rows = pl.ds(*groups[g]), pl.ds(o0 * SUB, on * SUB)
        arrived(rx.at[js, pl.ds(half, nx - 1), rows], d2.at[b, g])
        for d in range(1, nx):
            block = rx.at[js, half + x_at(-d), rows]
            send(block, block, ssem.at[2], d3.at[b, g], me_n, partner)

    def hidden(b, g):
        o0, on = batches[b]
        j0, jn = groups[g]
        m = n_local * on * SUB
        arrived(rx.at[pl.ds(j0, jn), pl.ds(other, nx), pl.ds(o0 * SUB, on * SUB)], d3.at[b, g])
        if b == 0 and g == 0:
            pltpu.make_async_copy(wgu, wgu, psem.at[0]).wait()
        x = jnp.concatenate([
            from_tiles(rx[j, :, o0 * SUB:(o0 + on) * SUB].reshape(m, SUB, LANE), m, j % 2)
            for j in range(j0, j0 + jn)], axis=1)
        ks = pl.ds(j0 * COLS, jn * COLS)
        both = jnp.concatenate([wgu[i, ks, :] for i in range(2 * ff // LANE)], axis=1)
        now = jnp.dot(x, both, preferred_element_type=f32)
        sums[b] = sums[b] + now if b in sums else now
        if g == len(groups) - 1:
            gate, up = sums[b][:, 0:ff], sums[b][:, ff:2 * ff]
            inner[b] = (gate / (1.0 + jnp.exp(-gate)) * up).astype(bf16)

    def down(b, g):
        o0, on = batches[b]
        j0, jn = groups[g]
        if b == 0 and g == 0:
            loads[0].wait()
        for j in range(j0, j0 + jn):
            y = jnp.dot(inner[b], wd[:, j * COLS:(j + 1) * COLS], preferred_element_type=f32)
            py[j, :, o0:o0 + on] = y.reshape(n_local, on, SUB, COLS).astype(bf16)
        js = pl.ds(j0, jn)
        send(py.at[js, pl.ds(other, nx), pl.ds(o0, on)], r1b.at[js, :, pl.ds(o0, on)],
             ssem.at[3], d1.at[b, g, 0], me_n, partner)

    def pair_sum(b, g):
        o0, on = batches[b]
        j0, jn = groups[g]
        js, os = pl.ds(j0, jn), pl.ds(o0, on)
        arrived(r1b.at[js, :, os], d1.at[b, g, 0])
        for d in range(1, nx):
            xd = x_at(d)
            for j in range(j0, j0 + jn):
                s2[j, d - 1, o0:o0 + on] = (py[j, half + xd, o0:o0 + on].astype(f32)
                                            + r1b[j, xd, o0:o0 + on].astype(f32)).astype(bf16)
            send(s2.at[js, d - 1, os], r2b.at[js, d - 1, os], ssem.at[4], d1.at[b, g, 1], me_n, xd * 2 + me_c)

    def answer(b, g):
        o0, on = batches[b]
        j0, jn = groups[g]
        js, os = pl.ds(j0, jn), pl.ds(o0, on)
        arrived(r2b.at[js, :, os], d1.at[b, g, 1])
        for j in range(j0, j0 + jn):
            total = py[j, mine, o0:o0 + on].astype(f32) + r1b[j, me_x, o0:o0 + on].astype(f32)
            for d in range(1, nx):
                total = total + r2b[j, d - 1, o0:o0 + on].astype(f32)
            tiles = to_tiles(total.reshape(on * SUB, COLS), on * SUB, j % 2)
            a3[j, o0 * SUB:(o0 + on) * SUB] = tiles
            for p, n in own_rows(b):
                ax[j, p:p + n] = tiles[p - o0 * SUB:p - o0 * SUB + n]
        send_back(b, g)

    run = {"pass_near": functools.partial(pass_part, far=False), "pass_far": functools.partial(pass_part, far=True), "pass_across": pass_across, "hidden": hidden, "down": down,
           "pair_sum": pair_sum, "answer": answer}
    for name, b, g in plan([on for _, on in batches], len(groups)):
        with jax.named_scope(f"{name}_{b}{g}"):
            run[name](b, g)
        if (name, b, g) == ("pass_far", 0, len(groups) - 1):
            for late in range(EARLY, len(batches)):
                for i in range(len(groups)):
                    send_out(late, i)
    for g, (j0, jn) in enumerate(groups):
        with jax.named_scope(f"back_{g}"):
            arrived(ax.at[pl.ds(j0, jn), pl.ds(0, per - SLOT)], c3.at[g])
        for j in range(j0, j0 + jn):
            answers = from_tiles(ax[j], per, j % 2, 2)
            out_ref[:, j * COLS:(j + 1) * COLS] = jnp.dot(place, answers, preferred_element_type=f32).astype(bf16)
    for i, ref in enumerate((tx.at[:, pl.ds(0, per - SLOT)], rx.at[:, pl.ds(0, nx - 1)], rx.at[:, pl.ds(0, nx)],
                             py.at[:, pl.ds(0, nx)], s2, a3.at[:, pl.ds(0, per - SLOT)])):
        remote(ref, ref, ssem.at[i], ssem.at[i], me_n, partner).wait_send()


def shards(n_node, n_local, tokens, w_gate, w_up, w_down, chosen, counts, gates):
    tok_dev, width = tokens.shape
    ff = w_gate.shape[2]
    chunks = width // COLS
    nx = n_local // 2
    per = n_node * SLOT
    octs = per // SUB
    nb, ng = len(batches_of(n_node)), len(split(chunks, GROUPS))
    deep = max(per, n_local * SUB * batches_of(n_node)[-1][1])
    bf16 = jnp.bfloat16
    vmem = pl.BlockSpec(memory_space=pltpu.VMEM)
    dma = pltpu.SemaphoreType.DMA
    buffers = [
        ((tok_dev, width), bf16),
        ((2 * ff // LANE, width, LANE), bf16),
        ((ff, width), bf16),
        ((chunks, per, SUB, LANE), bf16),
        ((chunks, n_local, per, SUB, LANE), bf16),
        ((chunks, n_local, octs, SUB, COLS), bf16),
        ((chunks, nx, octs, SUB, COLS), bf16),
        ((chunks, nx - 1, octs, SUB, COLS), bf16),
        ((chunks, nx - 1, octs, SUB, COLS), bf16),
        ((chunks, per, SUB, LANE), bf16),
        ((chunks, per, SUB, LANE), bf16),
        ((2, deep * SUB, LANE), jnp.float32),
    ]
    size = sum(functools.reduce(lambda a, b: a * b, shape) * jnp.dtype(kind).itemsize for shape, kind in buffers)
    args = (counts, chosen, gates, tokens, w_gate, w_up, w_down)
    return pl.pallas_call(
        functools.partial(kernel, (n_node, n_local, chunks, tok_dev, ff)),
        out_shape=jax.ShapeDtypeStruct((tok_dev, width), bf16),
        in_specs=[pl.BlockSpec(memory_space=pl.ANY)] * 7,
        out_specs=vmem,
        scratch_shapes=[
            pltpu.SMEM(counts.shape, counts.dtype),
            pltpu.VMEM(chosen.shape, chosen.dtype),
            pltpu.VMEM(gates.shape, gates.dtype),
            *(pltpu.VMEM(shape, kind) for shape, kind in buffers),
            dma((4 + ng,)), dma((1,)), dma((6,)),
            dma((nb, ng, 2)), dma((nb, ng)), dma((nb, ng)), dma((ng,)),
        ],
        compiler_params=pltpu.CompilerParams(
            collective_id=0, has_side_effects=True, vmem_limit_bytes=min(size + 14000000, 66000000)),
    )(*(pltpu.with_memory_space_constraint(arg, pltpu.HBM) for arg in args))


def solution(mesh):
    in_specs = (
        P(("node", "local"), None),
        P("node", None, "local"),
        P("node", None, "local"),
        P("node", "local", None),
        P(),
        P(),
        P(),
    )
    out_specs = P(("node", "local"), None)
    body = functools.partial(shards, mesh.shape["node"], mesh.shape["local"])
    return jax.shard_map(body, mesh=mesh, in_specs=in_specs, out_specs=out_specs, check_vma=False)
```
